32 devices in a mesh: replica: 8 (over z, x), tensor: 4 (over y, core).
Axes of the slice: x: 2, y: 2, z: 4, core: 2. Of those that a mesh axis runs over, the one named last changes fastest.
Arguments:
- queries: bfloat16 [512, 8192], P('replica', 'tensor'), may hold values from -18 to 18
- kv_new: bfloat16 [512, 2, 1024], P('replica', None, 'tensor'), may hold values from -7.5 to 7.5
- pool: bfloat16 [192, 128, 2, 1024], P('replica', None, None, 'tensor'), may hold values from -240 to 240
- page_table: int32 [16, 12], P('replica'), may hold values from 0 to 191, as said below
- hist_len: int32 [16], P('replica'), may hold values from 769 to 1536
- o_weight: bfloat16 [8192, 8192], P('tensor'), may hold values from -0.125 to 0.125
Outputs:
- mixed: bfloat16 [512, 8192], P(('replica', 'tensor'))
The draws below stay inside these ranges and needn't reach their ends.
Inputs may be any that keep to these rules, and one draw needn't show every extreme that they name: `page_table`: no two entries are equal. The owner of page id g is the replica group g // 24. Among the live pages (entry j of conversation c with j * 128 < hist_len[c]) of the conversations of one replica group, at most 3 have any one owner, and in every group some owner holds exactly 3 of them.
All inputs are finite; a program needn't handle non-finite values.
Results may differ from the reference program's by a relative error of at most 0.014.
Values may be sent and summed in bfloat16 or wider, within the bound.
A program may use at most 128 MiB of HBM per device.

```python
import math
import jax
import jax.numpy as jnp
from jax import lax

HEADS = 64
KV_HEADS = 8
HD = 128
D = 8192
NEW = 32
CONV_DEV = 2
PAGE = 128
MAXP = 12
SLOT = 3
CONVS = 16
TOKENS = 512
POOL_DEV = 24
POOL_PAGES = 192
N_TENSOR = 4


def draw_pool(key, part):
    base = jax.random.truncated_normal(key, -6.0, 6.0, (POOL_PAGES, PAGE, 2, KV_HEADS * HD), jnp.float32)
    return base.astype(jnp.bfloat16)


def draw_page_table(key, part):
    groups = CONVS // CONV_DEV
    width = groups * SLOT
    shelves = jax.vmap(lambda owner: jax.random.permutation(jax.random.fold_in(key, 5000 + owner), POOL_DEV))(jnp.arange(groups, dtype=jnp.int32))

    def one_group(group):
        sub = jax.random.fold_in(key, group)
        first = jax.random.randint(jax.random.fold_in(sub, 1), (), 0, groups)
        shuffled = jax.random.permutation(jax.random.fold_in(sub, 2), width).astype(jnp.int32)
        owner_of = jnp.arange(width, dtype=jnp.int32) // SLOT
        score = shuffled - width * (owner_of == first).astype(jnp.int32)
        chosen = jnp.argsort(score, stable=True)[:CONV_DEV * MAXP].astype(jnp.int32)
        owners = chosen // SLOT
        within = chosen % SLOT
        shelf = shelves[owners, group * SLOT + within]
        table = (owners * POOL_DEV + shelf).reshape(CONV_DEV, MAXP)
        front = jax.random.permutation(jax.random.fold_in(sub, 3), MAXP // 2)
        table = table.at[:, :MAXP // 2].set(table[:, front])
        turn = jax.random.randint(jax.random.fold_in(sub, 4), (), 0, CONV_DEV)
        return jnp.roll(table, turn, axis=0)
    return jax.vmap(one_group)(jnp.arange(groups, dtype=jnp.int32)).reshape(CONVS, MAXP).astype(jnp.int32)


def set_ends(entries, own_key, smallest, high):
    extent = entries.shape
    index_at = [jax.random.randint(jax.random.fold_in(own_key, axis), (), 0, extent[axis]) for axis in range(len(extent))]
    entries = entries.at[tuple(index_at)].set(smallest)
    longest = extent.index(max(extent))
    index_at[longest] = (index_at[longest] + 1) % extent[longest]
    return entries.at[tuple(index_at)].set(high)


def level_of(stream_key, dims, pieces, least, top_value):
    def one(position, shards_of):
        heights = jax.random.uniform(jax.random.fold_in(jax.random.fold_in(stream_key, 6), position), (shards_of,), jnp.float32, least / len(pieces), top_value / len(pieces))
        return jnp.repeat(jnp.exp(heights), dims[position] // shards_of).reshape((-1,) + (1,) * (len(dims) - position - 1))

    gain = one(*pieces[0])
    for cut in pieces[1:]:
        gain = gain * one(*cut)
    return gain


def normal_values(stream_key, shape, spread, limit, shards=(), kind=jnp.bfloat16):
    loudness = level_of(stream_key, shape, shards, -0.22, 0.18) if shards else 1.0
    values = jax.random.normal(stream_key, shape, jnp.float32) * spread * loudness
    return jnp.minimum(jnp.maximum(values, -limit), limit).astype(kind)


def setup_inputs(seed: int = 0) -> dict:
    arg_keys = jax.random.split(jax.random.key(seed), 7)
    return {
        "queries": normal_values(arg_keys[0], (TOKENS, HEADS * HD), 3.0, 18.0, ((0, 8), (1, 4))),
        "kv_new": normal_values(arg_keys[1], (TOKENS, 2, KV_HEADS * HD), 1.25, 7.5, ((0, 8), (2, 4))),
        "pool": draw_pool(jax.random.fold_in(arg_keys[6], 71), 0),
        "page_table": draw_page_table(jax.random.fold_in(arg_keys[6], 71), 0),
        "hist_len": set_ends(jax.random.randint(arg_keys[4], (CONVS,), MAXP * PAGE // 2 + 1, MAXP * PAGE + 1), jax.random.fold_in(arg_keys[4], 1), MAXP * PAGE // 2 + 1, MAXP * PAGE).astype(jnp.int32),
        "o_weight": normal_values(arg_keys[5], (HEADS * HD, D), (HEADS * HD // 4) ** -0.5, 0.125, ((0, 4),)),
    }


floor_value = -1e+30

def attend_part(asked, keys, values, allowed):
    scores = jnp.einsum('nkgd,tkd->nkgt', asked.astype(jnp.float32), keys.astype(jnp.float32)) / math.sqrt(HD)
    peak = lax.optimization_barrier(jnp.max(jnp.where(allowed, scores, floor_value), axis=-1))
    weights = jnp.where(allowed, jnp.exp(scores - peak[..., None]), 0.0).astype(jnp.bfloat16)
    weights = lax.optimization_barrier(weights).astype(jnp.float32)
    amount = lax.optimization_barrier(jnp.sum(weights, axis=-1))
    summed = jnp.einsum('nkgt,tkd->nkgd', weights, values.astype(jnp.float32))
    return (peak, amount, summed)

def merge(first, second):
    peak = jnp.maximum(first[0], second[0])
    keep = jnp.exp(first[0] - peak)
    take = jnp.exp(second[0] - peak)
    return (peak, keep * first[1] + take * second[1], keep[..., None] * first[2] + take[..., None] * second[2])

def reference(queries, kv_new, pool, page_table, hist_len, o_weight):
    per_group = HEADS // KV_HEADS
    asked_all = queries.reshape(CONVS, NEW, KV_HEADS, per_group, HD)
    fresh_all = kv_new.reshape(CONVS, NEW, 2, KV_HEADS, HD)
    pool_all = pool.reshape(POOL_PAGES, PAGE, 2, KV_HEADS, HD)
    order = jnp.arange(NEW, dtype=jnp.int32)
    causal = (order[None, :] <= order[:, None])[:, None, None, :]
    inside = jnp.arange(PAGE, dtype=jnp.int32)

    def one_dialog(items):
        asked, fresh, table, length = items
        state = attend_part(asked, fresh[:, 0], fresh[:, 1], causal)

        def step(carry, index):
            page = pool_all[table[index]]
            live = index * PAGE + inside < length
            part = attend_part(asked, page[:, 0], page[:, 1], live[None, None, None, :])
            used = index * PAGE < length
            merged = merge(carry, part)
            return (jax.tree.map(lambda fresh_value, old_value: jnp.where(used, fresh_value, old_value), merged, carry), None)
        state, _ = lax.scan(step, state, jnp.arange(MAXP, dtype=jnp.int32))
        attended = (state[2] / state[1][..., None]).astype(jnp.bfloat16)
        return attended.reshape(NEW, HEADS * HD)
    attended = lax.map(one_dialog, (asked_all, fresh_all, page_table, hist_len)).reshape(TOKENS, N_TENSOR, HEADS * HD // N_TENSOR)
    blocks = o_weight.reshape(N_TENSOR, HEADS * HD // N_TENSOR, D)

    def add_block(running, index):
        part = jnp.dot(attended[:, index], blocks[index], preferred_element_type=jnp.float32)
        part = lax.optimization_barrier(part.astype(jnp.bfloat16)).astype(jnp.float32)
        return (running + part, None)
    running, _ = lax.scan(add_block, jnp.zeros((TOKENS, D), jnp.float32), jnp.arange(N_TENSOR, dtype=jnp.int32))
    return running.astype(jnp.bfloat16)
```

```python
import functools
import math

import jax
import jax.numpy as jnp
from jax import lax
from jax.experimental import pallas as pl
from jax.experimental.pallas import tpu as pltpu
from jax.sharding import PartitionSpec as P

HD = 128
PAGE = 128
SLOT = 3
TILE = 1024


floor_value = -1e30

MESH = pl.DeviceIdType.MESH


def kernel(
    groups, shards, new_len,
    dialog_ref, fill_ref, q_ref, fresh_ref, outgoing, weight,
    out_ref,
    arrived, wbuf, perm, qs, kbuf, vbuf, peak_ref, amount_ref, summed_ref, attended, part, landed,
    send_sem, recv_sem, own_sem, weight_sem, part_send, part_recv,
):
    me = lax.axis_index("replica")
    mine = lax.axis_index("tensor")
    token_rows = q_ref.shape[0]
    kv_count, rows, _ = qs.shape
    per_group = rows // token_rows
    slots = arrived.shape[1]
    tiles, _, block_rows, tile = part.shape
    scale = 1.0 / math.sqrt(HD)

    own = pltpu.make_async_copy(outgoing.at[me], arrived.at[0], own_sem)
    own.start()

    barrier = pltpu.get_barrier_semaphore()
    for step in range(1, groups):
        pl.semaphore_signal(
            barrier, inc=1, device_id={"replica": lax.rem(me + step, groups)}, device_id_type=MESH
        )
    for step in range(1, shards):
        pl.semaphore_signal(
            barrier, inc=1, device_id={"tensor": lax.rem(mine + step, shards)}, device_id_type=MESH
        )
    pl.semaphore_wait(barrier, groups + shards - 2)

    def page_copy(step):
        dest = lax.rem(me + step, groups)
        return pltpu.make_async_remote_copy(
            src_ref=outgoing.at[dest],
            dst_ref=arrived.at[step],
            send_sem=send_sem.at[step],
            recv_sem=recv_sem.at[step],
            device_id={"replica": dest},
            device_id_type=MESH,
        )

    def weight_copy(index):
        return pltpu.make_async_copy(
            weight.at[:, pl.ds(pl.multiple_of(index * tile, tile), tile)],
            wbuf.at[index],
            weight_sem.at[index],
        )

    def part_copy(index, step):
        dest = lax.rem(mine + step, shards)
        return pltpu.make_async_remote_copy(
            src_ref=part.at[index, dest],
            dst_ref=landed.at[index, step - 1],
            send_sem=part_send.at[index, step - 1],
            recv_sem=part_recv.at[index, step - 1],
            device_id={"tensor": dest},
            device_id_type=MESH,
        )

    for step in range(1, groups):
        page_copy(step).start()
    for index in range(tiles):
        weight_copy(index).start()

    width = perm.shape[0]
    i = lax.broadcasted_iota(jnp.int32, (width, width), 0)
    j = lax.broadcasted_iota(jnp.int32, (width, width), 1)
    source = jnp.where(i < PAGE, 2 * i, 2 * (i - PAGE) + 1)
    perm[...] = jnp.where(source == j, 1.0, 0.0).astype(perm.dtype)

    for k in range(kv_count):
        for g in range(per_group):
            col = (k * per_group + g) * HD
            qs[k, g * token_rows : (g + 1) * token_rows, :] = q_ref[:, col : col + HD]

    contract = (((1,), (1,)), ((), ()))

    row_token = lax.broadcasted_iota(jnp.int32, (rows, token_rows), 0) % token_rows
    col_token = lax.broadcasted_iota(jnp.int32, (rows, token_rows), 1)
    causal = (row_token // new_len == col_token // new_len) & (col_token <= row_token)
    for k in range(kv_count):
        keys = fresh_ref[0, :, k * HD : (k + 1) * HD]
        values = fresh_ref[1, :, k * HD : (k + 1) * HD]
        scores = lax.dot_general(qs[k], keys, contract, preferred_element_type=jnp.float32) * scale
        scores = jnp.where(causal, scores, floor_value)
        peak = jnp.max(scores, axis=-1, keepdims=True)
        weights = jnp.exp(scores - peak).astype(jnp.bfloat16)
        peak_ref[k] = jnp.broadcast_to(peak, (rows, HD))
        amount_ref[k] = jnp.broadcast_to(
            jnp.sum(weights.astype(jnp.float32), axis=-1, keepdims=True), (rows, HD)
        )
        summed_ref[k] = jnp.dot(weights, values, preferred_element_type=jnp.float32)

    def absorb(step):
        owner = lax.rem(me - step + groups, groups)
        row_dialog = (
            lax.broadcasted_iota(jnp.int32, (rows, PAGE), 0) % token_rows
        ) // new_len
        position = lax.broadcasted_iota(jnp.int32, (rows, PAGE), 1)
        allowed = []
        for s in range(slots):
            split = jnp.dot(perm[...], arrived[step, s], preferred_element_type=jnp.float32)
            split = split.astype(jnp.bfloat16)
            kbuf[s * PAGE : (s + 1) * PAGE, :] = split[:PAGE]
            vbuf[s * PAGE : (s + 1) * PAGE, :] = split[PAGE:]
            limit = jnp.where(row_dialog == dialog_ref[owner, s], fill_ref[owner, s], 0)
            allowed.append(position < limit)
        for k in range(kv_count):
            keys = kbuf[:, k * HD : (k + 1) * HD]
            values = vbuf[:, k * HD : (k + 1) * HD]
            scores = (
                lax.dot_general(qs[k], keys, contract, preferred_element_type=jnp.float32) * scale
            )
            pieces = [
                jnp.where(allowed[s], scores[:, s * PAGE : (s + 1) * PAGE], floor_value)
                for s in range(slots)
            ]
            high = functools.reduce(jnp.maximum, pieces)
            before = peak_ref[k]
            peak = jnp.maximum(before, jnp.max(high, axis=-1, keepdims=True))
            keep = jnp.exp(before - peak)
            weights = [jnp.exp(piece - peak).astype(jnp.bfloat16) for piece in pieces]
            added = functools.reduce(jnp.add, [w.astype(jnp.float32) for w in weights])
            peak_ref[k] = peak
            amount_ref[k] = keep * amount_ref[k] + jnp.sum(added, axis=-1, keepdims=True)
            summed_ref[k] = keep * summed_ref[k] + jnp.dot(
                jnp.concatenate(weights, axis=1), values, preferred_element_type=jnp.float32
            )

    own.wait()
    absorb(0)

    def page_step(step, carry):
        page_copy(step).wait_recv()
        absorb(step)
        return carry

    lax.fori_loop(1, groups, page_step, 0)

    for k in range(kv_count):
        for g in range(per_group):
            span = slice(g * token_rows, (g + 1) * token_rows)
            col = (k * per_group + g) * HD
            attended[:, col : col + HD] = (summed_ref[k, span] / amount_ref[k, span]).astype(
                jnp.bfloat16
            )

    def project(index, carry):
        weight_copy(index).wait()
        product = jnp.dot(attended[...], wbuf[index], preferred_element_type=jnp.float32)
        part[index] = product.astype(jnp.bfloat16).reshape(shards, block_rows, tile)
        for step in range(1, shards):
            part_copy(index, step).start()
        return carry

    lax.fori_loop(0, tiles, project, 0)

    def finish(index, carry):
        total = part[index, mine].astype(jnp.float32)
        for step in range(1, shards):
            part_copy(index, step).wait_recv()
            total = total + landed[index, step - 1].astype(jnp.float32)
        out_ref[:, pl.ds(pl.multiple_of(index * tile, tile), tile)] = total.astype(out_ref.dtype)
        return carry

    lax.fori_loop(0, tiles, finish, 0)

    def drain(index, carry):
        for step in range(1, shards):
            part_copy(index, step).wait_send()
        return carry

    lax.fori_loop(0, tiles, drain, 0)
    for step in range(1, groups):
        page_copy(step).wait_send()


def request_lists(page_table, hist_len, groups, pool_size):
    dialogs, entries = page_table.shape
    position = jnp.arange(entries, dtype=jnp.int32)
    fills = jnp.clip(hist_len[:, None] - position[None, :] * PAGE, 0, PAGE).reshape(-1)
    owners = (page_table // pool_size).reshape(-1)
    shelf = (page_table % pool_size).reshape(-1)
    dialog_of = jnp.repeat(jnp.arange(dialogs, dtype=jnp.int32), entries)
    hits = (owners[:, None] == jnp.arange(groups, dtype=jnp.int32)[None, :]) & (fills > 0)[:, None]
    ranks = jnp.cumsum(hits.astype(jnp.int32), axis=0) - 1
    places = hits.T[:, None, :] & (
        ranks.T[:, None, :] == jnp.arange(SLOT, dtype=jnp.int32)[None, :, None]
    )
    picked = places.astype(jnp.int32)
    wanted = jnp.sum(picked * shelf[None, None, :], axis=-1)
    dialog_ids = jnp.sum(picked * dialog_of[None, None, :], axis=-1)
    slot_fill = jnp.sum(picked * fills[None, None, :], axis=-1)
    return (wanted, dialog_ids, slot_fill)


def local(queries, kv_new, pool, page_table, hist_len, o_weight):
    groups = lax.axis_size("replica")
    shards = lax.axis_size("tensor")
    pool_size, page_len, _, kv_width = pool.shape
    dialogs = page_table.shape[0]
    token_rows = queries.shape[0]
    new_len = token_rows // dialogs
    kv_count = kv_width // HD
    per_group = queries.shape[1] // kv_width
    rows = per_group * token_rows
    depth, model = o_weight.shape
    tile = min(TILE, model)
    tiles = model // tile
    block_rows = token_rows // shards
    wanted, dialog_ids, slot_fill = request_lists(page_table, hist_len, groups, pool_size)
    shelf_ids = lax.all_to_all(wanted, "replica", split_axis=0, concat_axis=0, tiled=True)
    outgoing = pool[shelf_ids].reshape(groups, SLOT, 2 * page_len, kv_width)
    fresh = jnp.stack([kv_new[:, 0], kv_new[:, 1]])
    vmem = pl.BlockSpec(memory_space=pltpu.VMEM)
    smem = pl.BlockSpec(memory_space=pltpu.SMEM)
    anywhere = pl.BlockSpec(memory_space=pl.ANY)
    return pl.pallas_call(
        functools.partial(kernel, groups, shards, new_len),
        out_shape=jax.ShapeDtypeStruct((block_rows, model), jnp.bfloat16),
        in_specs=[smem, smem, vmem, vmem, anywhere, anywhere],
        out_specs=vmem,
        scratch_shapes=[
            pltpu.VMEM((groups, SLOT, 2 * page_len, kv_width), jnp.bfloat16),
            pltpu.VMEM((tiles, depth, tile), jnp.bfloat16),
            pltpu.VMEM((2 * page_len, 2 * page_len), jnp.bfloat16),
            pltpu.VMEM((kv_count, rows, HD), jnp.bfloat16),
            pltpu.VMEM((SLOT * page_len, kv_width), jnp.bfloat16),
            pltpu.VMEM((SLOT * page_len, kv_width), jnp.bfloat16),
            pltpu.VMEM((kv_count, rows, HD), jnp.float32),
            pltpu.VMEM((kv_count, rows, HD), jnp.float32),
            pltpu.VMEM((kv_count, rows, HD), jnp.float32),
            pltpu.VMEM((token_rows, depth), jnp.bfloat16),
            pltpu.VMEM((tiles, shards, block_rows, tile), jnp.bfloat16),
            pltpu.VMEM((tiles, shards - 1, block_rows, tile), jnp.bfloat16),
            pltpu.SemaphoreType.DMA((groups,)),
            pltpu.SemaphoreType.DMA((groups,)),
            pltpu.SemaphoreType.DMA,
            pltpu.SemaphoreType.DMA((tiles,)),
            pltpu.SemaphoreType.DMA((tiles, shards - 1)),
            pltpu.SemaphoreType.DMA((tiles, shards - 1)),
        ],
        compiler_params=pltpu.CompilerParams(
            collective_id=0, has_side_effects=True, vmem_limit_bytes=60 * 1024 * 1024
        ),
        name="attend",
    )(dialog_ids, slot_fill, queries, fresh, outgoing, o_weight)


def solution(mesh):
    in_specs = (
        P("replica", "tensor"),
        P("replica", None, "tensor"),
        P("replica", None, None, "tensor"),
        P("replica", None),
        P("replica"),
        P("tensor", None),
    )
    out_specs = P(("replica", "tensor"), None)
    return jax.shard_map(local, mesh=mesh, in_specs=in_specs, out_specs=out_specs, check_vma=False)
```

```python
import functools
import math

import jax
import jax.numpy as jnp
from jax import lax
from jax.experimental import pallas as pl
from jax.experimental.pallas import tpu as pltpu
from jax.sharding import PartitionSpec as P

HD = 128
PAGE = 128
SLOT = 3
TILE = 1024


floor_value = -1e30

MESH = pl.DeviceIdType.MESH


def kernel(
    groups, shards, new_len,
    shelf_ref, dialog_ref, fill_ref, q_ref, fresh_ref, pool_ref, weight,
    out_ref,
    outgoing, arrived, wbuf, perm, qs, kbuf, vbuf, peak_ref, amount_ref, summed_ref, attended, part, landed,
    send_sem, recv_sem, weight_sem, part_send, part_recv,
):
    me = lax.axis_index("replica")
    mine = lax.axis_index("tensor")
    token_rows = q_ref.shape[0]
    kv_count, rows, _ = qs.shape
    per_group = rows // token_rows
    slots = arrived.shape[1]
    tiles, _, block_rows, tile = part.shape
    scale = 1.0 / math.sqrt(HD)

    barrier = pltpu.get_barrier_semaphore()
    for step in range(1, groups):
        pl.semaphore_signal(
            barrier, inc=1, device_id={"replica": lax.rem(me + step, groups)}, device_id_type=MESH
        )
    for step in range(1, shards):
        pl.semaphore_signal(
            barrier, inc=1, device_id={"tensor": lax.rem(mine + step, shards)}, device_id_type=MESH
        )

    def collect(step, carry):
        dest = lax.rem(me + step, groups)
        for s in range(slots):
            outgoing[step, s] = pool_ref[shelf_ref[dest, s]]
        return carry

    lax.fori_loop(0, groups, collect, 0)
    pl.semaphore_wait(barrier, groups + shards - 2)

    def page_copy(step):
        dest = lax.rem(me + step, groups)
        return pltpu.make_async_remote_copy(
            src_ref=outgoing.at[step],
            dst_ref=arrived.at[step],
            send_sem=send_sem.at[step],
            recv_sem=recv_sem.at[step],
            device_id={"replica": dest},
            device_id_type=MESH,
        )

    def weight_copy(index):
        return pltpu.make_async_copy(
            weight.at[:, pl.ds(pl.multiple_of(index * tile, tile), tile)],
            wbuf.at[index],
            weight_sem.at[index],
        )

    def part_copy(index, step):
        dest = lax.rem(mine + step, shards)
        return pltpu.make_async_remote_copy(
            src_ref=part.at[index, dest],
            dst_ref=landed.at[index, step - 1],
            send_sem=part_send.at[index, step - 1],
            recv_sem=part_recv.at[index, step - 1],
            device_id={"tensor": dest},
            device_id_type=MESH,
        )

    for step in range(1, groups):
        page_copy(step).start()
    for index in range(tiles):
        weight_copy(index).start()

    width = perm.shape[0]
    i = lax.broadcasted_iota(jnp.int32, (width, width), 0)
    j = lax.broadcasted_iota(jnp.int32, (width, width), 1)
    source = jnp.where(i < PAGE, 2 * i, 2 * (i - PAGE) + 1)
    perm[...] = jnp.where(source == j, 1.0, 0.0).astype(perm.dtype)

    for k in range(kv_count):
        for g in range(per_group):
            col = (k * per_group + g) * HD
            qs[k, g * token_rows : (g + 1) * token_rows, :] = q_ref[:, col : col + HD]

    contract = (((1,), (1,)), ((), ()))

    row_token = lax.broadcasted_iota(jnp.int32, (rows, token_rows), 0) % token_rows
    col_token = lax.broadcasted_iota(jnp.int32, (rows, token_rows), 1)
    causal = (row_token // new_len == col_token // new_len) & (col_token <= row_token)
    for k in range(kv_count):
        keys = fresh_ref[0, :, k * HD : (k + 1) * HD]
        values = fresh_ref[1, :, k * HD : (k + 1) * HD]
        scores = lax.dot_general(qs[k], keys, contract, preferred_element_type=jnp.float32) * scale
        scores = jnp.where(causal, scores, floor_value)
        peak = jnp.max(scores, axis=-1, keepdims=True)
        weights = jnp.exp(scores - peak).astype(jnp.bfloat16)
        peak_ref[k] = jnp.broadcast_to(peak, (rows, HD))
        amount_ref[k] = jnp.broadcast_to(
            jnp.sum(weights.astype(jnp.float32), axis=-1, keepdims=True), (rows, HD)
        )
        summed_ref[k] = jnp.dot(weights, values, preferred_element_type=jnp.float32)

    def absorb(step, pages):
        owner = lax.rem(me - step + groups, groups)
        row_dialog = (
            lax.broadcasted_iota(jnp.int32, (rows, PAGE), 0) % token_rows
        ) // new_len
        position = lax.broadcasted_iota(jnp.int32, (rows, PAGE), 1)
        allowed = []
        for s in range(slots):
            split = jnp.dot(perm[...], pages[step, s], preferred_element_type=jnp.float32)
            split = split.astype(jnp.bfloat16)
            kbuf[s * PAGE : (s + 1) * PAGE, :] = split[:PAGE]
            vbuf[s * PAGE : (s + 1) * PAGE, :] = split[PAGE:]
            limit = jnp.where(row_dialog == dialog_ref[owner, s], fill_ref[owner, s], 0)
            allowed.append(position < limit)
        for k in range(kv_count):
            keys = kbuf[:, k * HD : (k + 1) * HD]
            values = vbuf[:, k * HD : (k + 1) * HD]
            scores = (
                lax.dot_general(qs[k], keys, contract, preferred_element_type=jnp.float32) * scale
            )
            pieces = [
                jnp.where(allowed[s], scores[:, s * PAGE : (s + 1) * PAGE], floor_value)
                for s in range(slots)
            ]
            high = functools.reduce(jnp.maximum, pieces)
            before = peak_ref[k]
            peak = jnp.maximum(before, jnp.max(high, axis=-1, keepdims=True))
            keep = jnp.exp(before - peak)
            weights = [jnp.exp(piece - peak).astype(jnp.bfloat16) for piece in pieces]
            added = functools.reduce(jnp.add, [w.astype(jnp.float32) for w in weights])
            peak_ref[k] = peak
            amount_ref[k] = keep * amount_ref[k] + jnp.sum(added, axis=-1, keepdims=True)
            summed_ref[k] = keep * summed_ref[k] + jnp.dot(
                jnp.concatenate(weights, axis=1), values, preferred_element_type=jnp.float32
            )

    absorb(0, outgoing)

    def page_step(step, carry):
        page_copy(step).wait_recv()
        absorb(step, arrived)
        return carry

    lax.fori_loop(1, groups, page_step, 0)

    for k in range(kv_count):
        for g in range(per_group):
            span = slice(g * token_rows, (g + 1) * token_rows)
            col = (k * per_group + g) * HD
            attended[:, col : col + HD] = (summed_ref[k, span] / amount_ref[k, span]).astype(
                jnp.bfloat16
            )

    def project(index, carry):
        weight_copy(index).wait()
        product = jnp.dot(attended[...], wbuf[index], preferred_element_type=jnp.float32)
        part[index] = product.astype(jnp.bfloat16).reshape(shards, block_rows, tile)
        for step in range(1, shards):
            part_copy(index, step).start()
        return carry

    lax.fori_loop(0, tiles, project, 0)

    def finish(index, carry):
        total = part[index, mine].astype(jnp.float32)
        for step in range(1, shards):
            part_copy(index, step).wait_recv()
            total = total + landed[index, step - 1].astype(jnp.float32)
        out_ref[:, pl.ds(pl.multiple_of(index * tile, tile), tile)] = total.astype(out_ref.dtype)
        return carry

    lax.fori_loop(0, tiles, finish, 0)

    def drain(index, carry):
        for step in range(1, shards):
            part_copy(index, step).wait_send()
        return carry

    lax.fori_loop(0, tiles, drain, 0)
    for step in range(1, groups):
        page_copy(step).wait_send()


def request_lists(page_table, hist_len, groups, pool_size):
    dialogs, entries = page_table.shape
    position = jnp.arange(entries, dtype=jnp.int32)
    fills = jnp.clip(hist_len[:, None] - position[None, :] * PAGE, 0, PAGE).reshape(-1)
    owners = (page_table // pool_size).reshape(-1)
    shelf = (page_table % pool_size).reshape(-1)
    dialog_of = jnp.repeat(jnp.arange(dialogs, dtype=jnp.int32), entries)
    hits = (owners[:, None] == jnp.arange(groups, dtype=jnp.int32)[None, :]) & (fills > 0)[:, None]
    ranks = jnp.cumsum(hits.astype(jnp.int32), axis=0) - 1
    places = hits.T[:, None, :] & (
        ranks.T[:, None, :] == jnp.arange(SLOT, dtype=jnp.int32)[None, :, None]
    )
    picked = places.astype(jnp.int32)
    wanted = jnp.sum(picked * shelf[None, None, :], axis=-1)
    dialog_ids = jnp.sum(picked * dialog_of[None, None, :], axis=-1)
    slot_fill = jnp.sum(picked * fills[None, None, :], axis=-1)
    return (wanted, dialog_ids, slot_fill)


def local(queries, kv_new, pool, page_table, hist_len, o_weight):
    groups = lax.axis_size("replica")
    shards = lax.axis_size("tensor")
    pool_size, page_len, _, kv_width = pool.shape
    dialogs = page_table.shape[0]
    token_rows = queries.shape[0]
    new_len = token_rows // dialogs
    kv_count = kv_width // HD
    per_group = queries.shape[1] // kv_width
    rows = per_group * token_rows
    depth, model = o_weight.shape
    tile = min(TILE, model)
    tiles = model // tile
    block_rows = token_rows // shards
    wanted, dialog_ids, slot_fill = request_lists(page_table, hist_len, groups, pool_size)
    shelf_ids = lax.all_to_all(wanted, "replica", split_axis=0, concat_axis=0, tiled=True)
    pages = pool.reshape(pool_size, 2 * page_len, kv_width)
    fresh = jnp.stack([kv_new[:, 0], kv_new[:, 1]])
    vmem = pl.BlockSpec(memory_space=pltpu.VMEM)
    smem = pl.BlockSpec(memory_space=pltpu.SMEM)
    anywhere = pl.BlockSpec(memory_space=pl.ANY)
    return pl.pallas_call(
        functools.partial(kernel, groups, shards, new_len),
        out_shape=jax.ShapeDtypeStruct((block_rows, model), jnp.bfloat16),
        in_specs=[smem, smem, smem, vmem, vmem, vmem, anywhere],
        out_specs=vmem,
        scratch_shapes=[
            pltpu.VMEM((groups, SLOT, 2 * page_len, kv_width), jnp.bfloat16),
            pltpu.VMEM((groups, SLOT, 2 * page_len, kv_width), jnp.bfloat16),
            pltpu.VMEM((tiles, depth, tile), jnp.bfloat16),
            pltpu.VMEM((2 * page_len, 2 * page_len), jnp.bfloat16),
            pltpu.VMEM((kv_count, rows, HD), jnp.bfloat16),
            pltpu.VMEM((SLOT * page_len, kv_width), jnp.bfloat16),
            pltpu.VMEM((SLOT * page_len, kv_width), jnp.bfloat16),
            pltpu.VMEM((kv_count, rows, HD), jnp.float32),
            pltpu.VMEM((kv_count, rows, HD), jnp.float32),
            pltpu.VMEM((kv_count, rows, HD), jnp.float32),
            pltpu.VMEM((token_rows, depth), jnp.bfloat16),
            pltpu.VMEM((tiles, shards, block_rows, tile), jnp.bfloat16),
            pltpu.VMEM((tiles, shards - 1, block_rows, tile), jnp.bfloat16),
            pltpu.SemaphoreType.DMA((groups,)),
            pltpu.SemaphoreType.DMA((groups,)),
            pltpu.SemaphoreType.DMA((tiles,)),
            pltpu.SemaphoreType.DMA((tiles, shards - 1)),
            pltpu.SemaphoreType.DMA((tiles, shards - 1)),
        ],
        compiler_params=pltpu.CompilerParams(
            collective_id=0, has_side_effects=True, vmem_limit_bytes=63 * 1024 * 1024
        ),
        name="attend",
    )(shelf_ids, dialog_ids, slot_fill, queries, fresh, pages, o_weight)


def solution(mesh):
    in_specs = (
        P("replica", "tensor"),
        P("replica", None, "tensor"),
        P("replica", None, None, "tensor"),
        P("replica", None),
        P("replica"),
        P("tensor", None),
    )
    out_specs = P(("replica", "tensor"), None)
    return jax.shard_map(local, mesh=mesh, in_specs=in_specs, out_specs=out_specs, check_vma=False)
```
